32 devices in a mesh: row: 4 (over y, core), col: 8 (over z, x).
Axes of the slice: x: 2, y: 2, z: 4, core: 2. Of those that a mesh axis runs over, the one named last changes fastest.
Arguments:
- features: bfloat16 [32768, 128], P(('row', 'col')), may hold values from -6 to 6
- weight: bfloat16 [128, 128], replicated, may hold values from -0.5 to 0.5
- adj_tiles: bfloat16 [3072, 128, 128], P(('row', 'col')), may hold values from -0.21875 to 0.21875
- tile_rows: int32 [3072], P(('row', 'col')), may hold values from 0 to 63
- tile_cols: int32 [3072], P(('row', 'col')), may hold values from 0 to 31
- tile_count: int32 [32], P(('row', 'col')), may hold values from 24 to 96, as said below
- cotangent: bfloat16 [32768, 128], P(('row', 'col')), may hold values from -6 to 6
Outputs:
- out_features: bfloat16 [32768, 128], P(('row', 'col'))
- weight_grad: float32 [128, 128], replicated
- feature_grad: bfloat16 [32768, 128], P(('row', 'col'))
The draws below stay inside these ranges and needn't reach their ends.
Inputs may be any that keep to these rules, and one draw needn't show every extreme that they name: Each device has 96 slots, of which the first tile_count are in use; in every draw all devices of at least one row panel use all 96 slots.
All inputs are finite; a program needn't handle non-finite values.
Results may differ from the reference program's by a relative error of at most 0.019.
Values may be sent and summed in bfloat16 or wider, within the bound.
No kernel may reach another device: no remote copies, remote signals or barrier semaphores. Data moves between devices by JAX's collectives and lax.ppermute only.
A program may use at most 128 MiB of HBM per device.

```python
import jax
import jax.numpy as jnp
from jax import lax

F = 128
TILE = 128
NODE_DEV = 1024
TILES_DEV = 96
NODES = 32768
PANEL_TILES = 64
GROUP_TILES = 32
ALL_TILES = 3072
N_ROW = 4
N_COL = 8
DEVICES = 32


def draw_tile_count(key, part):
    first_key, second_key = jax.random.split(jax.random.fold_in(key, 71))
    hub_panels = max(1, N_ROW // 8)
    ranking = jax.random.permutation(first_key, N_ROW)
    hub_flags = (ranking < hub_panels).astype(jnp.int32)
    device_flags = jnp.repeat(hub_flags, N_COL)
    light_counts = jax.random.randint(second_key, (DEVICES,), TILES_DEV // 4, TILES_DEV // 2 + 1)
    return jnp.where(device_flags == 1, TILES_DEV, light_counts).astype(jnp.int32)


def set_ends(drawn, key, low, top_value):
    longest = drawn.shape.index(max(drawn.shape))
    spots = []
    for shift in (0, 1):
        where = [jax.random.randint(jax.random.fold_in(key, axis), (), 0, length) for axis, length in enumerate(drawn.shape)]
        where[longest] = (where[longest] + shift) % drawn.shape[longest]
        spots.append(tuple(where))
    return drawn.at[spots[0]].set(low).at[spots[1]].set(top_value)


def steps_of(rng, dims, cuts, smallest, high):
    loudness, own = 1.0, jax.random.fold_in(rng, 6)
    for axis_at, parts in cuts:
        draws = jnp.exp(jax.random.uniform(jax.random.fold_in(own, axis_at), (parts,), jnp.float32, smallest / len(cuts), high / len(cuts)))
        loudness = loudness * jnp.repeat(draws, dims[axis_at] // parts).reshape([-1 if axis == axis_at else 1 for axis in range(len(dims))])
    return loudness


def scatter_about(rng, dims, scale, bound, pieces=(), held_as=jnp.bfloat16):
    factor_of = steps_of(rng, dims, pieces, -0.22, 0.18) if pieces else 1.0
    drawn = jax.random.normal(rng, dims, jnp.float32) * scale * factor_of
    return jnp.minimum(jnp.maximum(drawn, -bound), bound).astype(held_as)


def setup_inputs(seed: int = 0) -> dict:
    splits = jax.random.split(jax.random.key(seed), 8)
    features = scatter_about(splits[0], (NODES, F), 1.0, 6.0, ((0, 32),))
    weight = scatter_about(splits[1], (F, F), F ** -0.5, 0.5)
    adj_tiles = scatter_about(splits[2], (ALL_TILES, TILE, TILE), (TILES_DEV * TILE * TILE * 9 // (20 * NODE_DEV)) ** -0.5, 0.21875, ((0, 32),))
    tile_rows = set_ends(jax.random.randint(splits[3], (ALL_TILES,), 0, PANEL_TILES), jax.random.fold_in(splits[3], 1), 0, PANEL_TILES - 1).astype(jnp.int32)
    tile_cols = set_ends(jax.random.randint(splits[4], (ALL_TILES,), 0, GROUP_TILES), jax.random.fold_in(splits[4], 1), 0, GROUP_TILES - 1).astype(jnp.int32)
    tile_count = draw_tile_count(jax.random.fold_in(splits[7], 71), 0)
    cotangent = scatter_about(splits[6], (NODES, F), 1.0, 6.0, ((0, 32),))
    return dict(features=features, weight=weight, adj_tiles=adj_tiles, tile_rows=tile_rows, tile_cols=tile_cols, tile_count=tile_count, cotangent=cotangent)


def activate(value):
    return jax.nn.gelu(value, approximate=True)

def activate_grad(pre_act, upstream):
    _, pullback = jax.vjp(activate, pre_act)
    return pullback(upstream)[0]

def reference(features, weight, adj_tiles, tile_rows, tile_cols, tile_count, cotangent):
    node_blocks = features.reshape(N_ROW, N_COL, NODE_DEV, F)
    tile_values = adj_tiles.reshape(DEVICES, TILES_DEV, TILE, TILE)
    row_table = tile_rows.reshape(DEVICES, TILES_DEV)
    col_table = tile_cols.reshape(DEVICES, TILES_DEV)
    positions = jnp.arange(TILES_DEV, dtype=jnp.int32)

    def masked(device):
        usable = (positions < tile_count[device]).astype(jnp.float32)
        return tile_values[device].astype(jnp.float32) * usable[:, None, None]

    def forward_step(summed, device):
        panel_index = device // N_COL
        group_index = device % N_COL
        group_rows = lax.dynamic_index_in_dim(node_blocks, group_index, 1, keepdims=False)
        group_rows = group_rows.reshape(GROUP_TILES, TILE, F).astype(jnp.float32)
        product = jnp.einsum('bij,bjf->bif', masked(device), group_rows[col_table[device]])
        partial_sum = jnp.zeros((PANEL_TILES, TILE, F), jnp.float32).at[row_table[device]].add(product)
        return (summed.at[panel_index].add(partial_sum), None)
    devices_list = jnp.arange(DEVICES, dtype=jnp.int32)
    summed, _ = lax.scan(forward_step, jnp.zeros((N_ROW, PANEL_TILES, TILE, F), jnp.float32), devices_list)
    hidden = summed.reshape(NODES, F).astype(jnp.bfloat16)
    pre_act = jnp.dot(hidden, weight, preferred_element_type=jnp.float32)
    out_features = activate(pre_act).astype(jnp.bfloat16)
    pre_grad = activate_grad(pre_act, cotangent.astype(jnp.float32)).astype(jnp.bfloat16)
    weight_grad = jnp.dot(hidden.T, pre_grad, preferred_element_type=jnp.float32)
    hidden_grad = jnp.dot(pre_grad, weight.T, preferred_element_type=jnp.float32).astype(jnp.bfloat16)
    grad_panels = hidden_grad.reshape(N_ROW, PANEL_TILES, TILE, F).astype(jnp.float32)

    def backward_step(summed, device):
        panel_index = device // N_COL
        group_index = device % N_COL
        panel_grad = lax.dynamic_index_in_dim(grad_panels, panel_index, 0, keepdims=False)
        product = jnp.einsum('bij,bif->bjf', masked(device), panel_grad[row_table[device]])
        partial_sum = jnp.zeros((GROUP_TILES, TILE, F), jnp.float32).at[col_table[device]].add(product)
        return (summed.at[group_index].add(partial_sum), None)
    group_grads, _ = lax.scan(backward_step, jnp.zeros((N_COL, GROUP_TILES, TILE, F), jnp.float32), devices_list)
    feature_grad = group_grads.reshape(N_COL, N_ROW, NODE_DEV, F).transpose(1, 0, 2, 3).reshape(NODES, F)
    return (out_features, weight_grad, feature_grad.astype(jnp.bfloat16))
```

```python
import functools

import jax
import jax.numpy as jnp
from jax import lax
from jax.experimental import pallas as pl
from jax.experimental.pallas import tpu as pltpu
from jax.sharding import PartitionSpec as P

UNROLL = 4
F32 = jnp.float32
BF16 = jnp.bfloat16
GELU_SCALE = 0.7978845608028654
GELU_CUBIC = 0.044715


def permute_xor(value, axis, mask):
    size = lax.axis_size(axis)
    return lax.ppermute(value, axis, [(i, i ^ mask) for i in range(size)])


def gather_pieces(value, axis):
    size = lax.axis_size(axis)
    pieces = [None] * size
    pieces[0] = value
    for major in list(range(4, size, 2)) + [2]:
        if major < size:
            pieces[major] = permute_xor(value, axis, major)
    for major in [0] + list(range(4, size, 2)) + [2]:
        if major < size:
            pieces[major + 1] = permute_xor(pieces[major], axis, 1)
    return pieces


def scatter_pieces(parts, axis):
    size = len(parts)
    terms = [parts[0]]
    for major in list(range(4, size, 2)) + [2]:
        if major < size:
            received = permute_xor(parts[major + 1], axis, 1)
            joined = (parts[major].astype(F32) + received.astype(F32)).astype(BF16)
            terms.append(permute_xor(joined, axis, major))
    terms.append(permute_xor(parts[1], axis, 1))
    return terms


def all_sum(value, axes):
    for axis in axes:
        mask = 1
        while mask < lax.axis_size(axis):
            value = value + permute_xor(value, axis, mask)
            mask *= 2
    return value


def tile_kernel(n_src, n_out, tile_size, slots, to_rows, *refs):
    rows_ref, cols_ref, count_ref, ids_ref, adj_hbm = refs[:5]
    sources = refs[5 : 5 + n_src]
    outs = refs[5 + n_src : 5 + n_src + n_out]
    adj, source, acc, sems = refs[5 + n_src + n_out :]
    src_id = ids_ref[0]
    out_id = ids_ref[1]
    adj_copy = pltpu.make_async_copy(adj_hbm, adj, sems.at[n_src])
    adj_copy.start()
    copies = []
    for r in range(n_src):
        copy = pltpu.make_async_copy(sources[r], source.at[src_id ^ r], sems.at[r])
        copy.start()
        copies.append(copy)
    out_tiles = n_out * outs[0].shape[0]
    src_tiles = source.shape[1]
    acc[...] = jnp.zeros(acc.shape, F32)
    for copy in copies:
        copy.wait()
    adj_copy.wait()
    count = count_ref[0]

    def step(block, carry):
        products = []
        for u in range(UNROLL):
            slot = block * UNROLL + u
            at = jnp.minimum(slot, slots - 1)
            if to_rows:
                target, origin = rows_ref[at], cols_ref[at]
            else:
                target, origin = cols_ref[at], rows_ref[at]
            target = jnp.where(slot < count, target, out_tiles)
            piece = source[origin // src_tiles, origin % src_tiles]
            if to_rows:
                product = jnp.dot(adj[at], piece, preferred_element_type=F32)
            else:
                product = jnp.dot(piece, adj[at], preferred_element_type=F32)
            products.append((target, product))
        for target, product in products:
            acc[target] = acc[target] + product
        return carry

    lax.fori_loop(0, (count + UNROLL - 1) // UNROLL, step, 0)
    for r in range(n_out):
        tiles = outs[r].shape[0]
        outs[r][...] = acc[pl.ds((out_id ^ r) * tiles, tiles)].astype(BF16)


def tile_pass(rows, cols, count, ids, adj_tiles, pieces, n_out, out_tiles, to_rows):
    slots, tile_size, _ = adj_tiles.shape
    n_src = len(pieces)
    block = pieces[0].shape
    width = block[-1]
    smem = pl.BlockSpec(memory_space=pltpu.SMEM)
    hbm = pl.BlockSpec(memory_space=pl.ANY)
    vmem = pl.BlockSpec(memory_space=pltpu.VMEM)
    return pl.pallas_call(
        functools.partial(tile_kernel, n_src, n_out, tile_size, slots, to_rows),
        in_specs=[smem] * 4 + [hbm] * (1 + n_src),
        out_specs=[vmem] * n_out,
        out_shape=[jax.ShapeDtypeStruct((out_tiles, tile_size, width), BF16)] * n_out,
        scratch_shapes=[
            pltpu.VMEM(adj_tiles.shape, BF16),
            pltpu.VMEM((n_src,) + block, BF16),
            pltpu.VMEM((n_out * out_tiles + 1, tile_size, width), F32),
            pltpu.SemaphoreType.DMA((n_src + 1,)),
        ],
    )(rows, cols, count, ids, adj_tiles, *pieces)


def middle_kernel(n_terms, *refs):
    terms = refs[:n_terms]
    weight_ref, cot_ref, out_ref, grad_ref, wterm_ref = refs[n_terms:]
    weight = weight_ref[...]
    wterm = None
    for t in range(cot_ref.shape[0]):
        total = terms[0][t].astype(F32)
        for term in terms[1:]:
            total = total + term[t].astype(F32)
        hidden = total.astype(BF16)
        pre = jnp.dot(hidden, weight, preferred_element_type=F32)
        square = pre * pre
        tanh = jnp.tanh(GELU_SCALE * (pre + GELU_CUBIC * square * pre))
        half = 0.5 * (1.0 + tanh)
        out_ref[t] = (pre * half).astype(BF16)
        slope = half + 0.5 * pre * (1.0 - tanh * tanh) * (
            GELU_SCALE * (1.0 + 3.0 * GELU_CUBIC * square)
        )
        grad = (cot_ref[t].astype(F32) * slope).astype(BF16)
        grad_ref[t] = lax.dot_general(
            weight, grad, (((1,), (1,)), ((), ())), preferred_element_type=F32
        ).astype(BF16)
        part = lax.dot_general(
            hidden, grad, (((0,), (0,)), ((), ())), preferred_element_type=F32
        )
        wterm = part if wterm is None else wterm + part
    wterm_ref[...] = wterm


def middle(terms, weight, cotangent):
    return pl.pallas_call(
        functools.partial(middle_kernel, len(terms)),
        out_shape=[
            jax.ShapeDtypeStruct(cotangent.shape, BF16),
            jax.ShapeDtypeStruct(cotangent.shape, BF16),
            jax.ShapeDtypeStruct(weight.shape, F32),
        ],
    )(*terms, weight, cotangent)


def final_kernel(n_terms, *refs):
    terms, out_ref = refs[:n_terms], refs[n_terms]
    for t in range(out_ref.shape[0]):
        total = terms[0][t].astype(F32)
        for term in terms[1:]:
            total = total + term[t].astype(F32)
        out_ref[t] = total.T.astype(BF16)


def final(terms):
    return pl.pallas_call(
        functools.partial(final_kernel, len(terms)),
        out_shape=jax.ShapeDtypeStruct(terms[0].shape, BF16),
    )(*terms)


def shards(features, weight, adj_tiles, tile_rows, tile_cols, tile_count, cotangent):
    node_dev, width = features.shape
    tile_size = adj_tiles.shape[1]
    dev_tiles = node_dev // tile_size
    as_tiles = (dev_tiles, tile_size, width)
    row_id = lax.axis_index("row").astype(jnp.int32)
    col_id = lax.axis_index("col").astype(jnp.int32)
    table = (tile_rows, tile_cols, tile_count)
    group = gather_pieces(features.reshape(as_tiles), "row")
    parts = tile_pass(
        *table, jnp.stack([row_id, col_id]), adj_tiles, group, lax.axis_size("col"), dev_tiles, True
    )
    terms = scatter_pieces(parts, "col")
    out_features, grad, wterm = middle(terms, weight, cotangent.reshape(as_tiles))
    panel = gather_pieces(grad, "col")
    weight_grad = all_sum(wterm, ("row", "col"))
    parts = tile_pass(
        *table, jnp.stack([col_id, row_id]), adj_tiles, panel, lax.axis_size("row"), dev_tiles, False
    )
    feature_grad = final(scatter_pieces(parts, "row"))
    return (
        out_features.reshape(node_dev, width),
        weight_grad,
        feature_grad.reshape(node_dev, width),
    )


def solution(mesh):
    in_specs = (
        P(("row", "col"), None),
        P(),
        P(("row", "col"), None, None),
        P(("row", "col")),
        P(("row", "col")),
        P(("row", "col")),
        P(("row", "col"), None),
    )
    out_specs = (P(("row", "col"), None), P(), P(("row", "col"), None))
    return jax.shard_map(shards, mesh=mesh, in_specs=in_specs, out_specs=out_specs, check_vma=False)
```

```python
import functools

import jax
import jax.numpy as jnp
from jax import lax
from jax.experimental import pallas as pl
from jax.experimental.pallas import tpu as pltpu
from jax.sharding import PartitionSpec as P

UNROLL = 4
F32 = jnp.float32
BF16 = jnp.bfloat16
GELU_SCALE = 0.7978845608028654
GELU_CUBIC = 0.044715


def permute_xor(value, axis, mask):
    size = lax.axis_size(axis)
    return lax.ppermute(value, axis, [(i, i ^ mask) for i in range(size)])


def is_inner(index):
    return (index // 2) % 4 in (1, 2)


def permute_some(value, axis, mask, keep):
    size = lax.axis_size(axis)
    return lax.ppermute(value, axis, [(i, i ^ mask) for i in range(size) if keep(i)])


def is_outer(index):
    return not is_inner(index)


def gather_pieces(value, axis):
    size = lax.axis_size(axis)
    pieces = [None] * size
    pieces[0] = [value]
    if size == 8:
        pieces[4] = [permute_xor(value, axis, 4)]
        inner = permute_some(value, axis, 6, is_inner)
        pieces[2] = [permute_xor(value, axis, 2)]
        pieces[1] = [permute_xor(value, axis, 1)]
        outer = permute_some(pieces[4][0], axis, 2, is_inner)
        pieces[5] = [permute_xor(pieces[4][0], axis, 1)]
        pieces[3] = [permute_xor(pieces[2][0], axis, 1)]
        pieces[6] = [inner, outer]
        pieces[7] = [
            permute_some(inner, axis, 1, is_inner),
            permute_some(outer, axis, 1, is_outer),
        ]
        return pieces
    for major in range(2, size, 2):
        pieces[major] = [permute_xor(value, axis, major)]
    for major in range(0, size, 2):
        pieces[major + 1] = [permute_xor(pieces[major][0], axis, 1)]
    return pieces


def join(*values):
    total = values[0].astype(F32)
    for value in values[1:]:
        total = total + value.astype(F32)
    return total.astype(BF16)


def scatter_pieces(parts, axis):
    size = len(parts)
    if size == 8:
        received = {r: permute_xor(parts[r], axis, 1) for r in (7, 5, 3, 1)}
        far = join(parts[6], received[7])
        outer = permute_some(far, axis, 2, is_outer)
        inner = permute_some(far, axis, 6, is_inner)
        skip = permute_xor(join(parts[4], received[5], outer), axis, 4)
        near = permute_xor(join(parts[2], received[3]), axis, 2)
        return [parts[0], received[1], inner, skip, near]
    terms = [parts[0]]
    for major in range(2, size, 2):
        received = permute_xor(parts[major + 1], axis, 1)
        terms.append(permute_xor(join(parts[major], received), axis, major))
    terms.append(permute_xor(parts[1], axis, 1))
    return terms


def all_sum(value, axes):
    for axis in axes:
        mask = 1
        while mask < lax.axis_size(axis):
            value = value + permute_xor(value, axis, mask)
            mask *= 2
    return value


def tile_kernel(choices, n_out, slots, to_rows, *refs):
    n_src = len(choices)
    n_arrays = sum(choices)
    rows_ref, cols_ref, count_ref, ids_ref, adj_hbm = refs[:5]
    arrays = list(refs[5 : 5 + n_arrays])
    outs = refs[5 + n_arrays : 5 + n_arrays + n_out]
    adj, source, acc, sems = refs[5 + n_arrays + n_out :]
    src_id = ids_ref[0]
    out_id = ids_ref[1]
    adj_copy = pltpu.make_async_copy(adj_hbm, adj, sems.at[n_src])
    adj_copy.start()
    copies = []
    for r, choice in enumerate(choices):
        options = [
            pltpu.make_async_copy(arrays.pop(0), source.at[src_id ^ r], sems.at[r])
            for _ in range(choice)
        ]
        if choice == 1:
            options[0].start()
        else:
            pl.when(ids_ref[2] == 1)(options[0].start)
            pl.when(ids_ref[2] == 0)(options[1].start)
        copies.append(options[0])
    out_tiles = n_out * outs[0].shape[0]
    src_tiles = source.shape[1]
    acc[...] = jnp.zeros(acc.shape, F32)
    for copy in copies:
        copy.wait()
    adj_copy.wait()
    count = count_ref[0]

    def step(block, carry):
        products = []
        for u in range(UNROLL):
            slot = block * UNROLL + u
            at = jnp.minimum(slot, slots - 1)
            if to_rows:
                target, origin = rows_ref[at], cols_ref[at]
            else:
                target, origin = cols_ref[at], rows_ref[at]
            target = jnp.where(slot < count, target, out_tiles)
            piece = source[origin // src_tiles, origin % src_tiles]
            if to_rows:
                product = jnp.dot(adj[at], piece, preferred_element_type=F32)
            else:
                product = jnp.dot(piece, adj[at], preferred_element_type=F32)
            products.append((target, product))
        for target, product in products:
            acc[target] = acc[target] + product
        return carry

    lax.fori_loop(0, (count + UNROLL - 1) // UNROLL, step, 0)
    for r in range(n_out):
        tiles = outs[r].shape[0]
        outs[r][...] = acc[pl.ds((out_id ^ r) * tiles, tiles)].astype(BF16)


def tile_pass(rows, cols, count, ids, adj_tiles, pieces, n_out, out_tiles, to_rows):
    slots, tile_size, _ = adj_tiles.shape
    n_src = len(pieces)
    arrays = [array for piece in pieces for array in piece]
    block = arrays[0].shape
    width = block[-1]
    smem = pl.BlockSpec(memory_space=pltpu.SMEM)
    hbm = pl.BlockSpec(memory_space=pl.ANY)
    vmem = pl.BlockSpec(memory_space=pltpu.VMEM)
    return pl.pallas_call(
        functools.partial(tile_kernel, [len(piece) for piece in pieces], n_out, slots, to_rows),
        in_specs=[smem] * 4 + [hbm] * (1 + len(arrays)),
        out_specs=[vmem] * n_out,
        out_shape=[jax.ShapeDtypeStruct((out_tiles, tile_size, width), BF16)] * n_out,
        scratch_shapes=[
            pltpu.VMEM(adj_tiles.shape, BF16),
            pltpu.VMEM((n_src,) + block, BF16),
            pltpu.VMEM((n_out * out_tiles + 1, tile_size, width), F32),
            pltpu.SemaphoreType.DMA((n_src + 1,)),
        ],
    )(rows, cols, count, ids, adj_tiles, *arrays)


def middle_kernel(n_terms, *refs):
    terms = refs[:n_terms]
    weight_ref, cot_ref, out_ref, grad_ref, wterm_ref = refs[n_terms:]
    weight = weight_ref[...]
    wterm = None
    for t in range(cot_ref.shape[0]):
        total = terms[0][t].astype(F32)
        for term in terms[1:]:
            total = total + term[t].astype(F32)
        hidden = total.astype(BF16)
        pre = jnp.dot(hidden, weight, preferred_element_type=F32)
        square = pre * pre
        tanh = jnp.tanh(GELU_SCALE * (pre + GELU_CUBIC * square * pre))
        half = 0.5 * (1.0 + tanh)
        out_ref[t] = (pre * half).astype(BF16)
        slope = half + 0.5 * pre * (1.0 - tanh * tanh) * (
            GELU_SCALE * (1.0 + 3.0 * GELU_CUBIC * square)
        )
        grad = (cot_ref[t].astype(F32) * slope).astype(BF16)
        grad_ref[t] = lax.dot_general(
            weight, grad, (((1,), (1,)), ((), ())), preferred_element_type=F32
        ).astype(BF16)
        part = lax.dot_general(
            hidden, grad, (((0,), (0,)), ((), ())), preferred_element_type=F32
        )
        wterm = part if wterm is None else wterm + part
    wterm_ref[...] = wterm


def middle(terms, weight, cotangent):
    return pl.pallas_call(
        functools.partial(middle_kernel, len(terms)),
        out_shape=[
            jax.ShapeDtypeStruct(cotangent.shape, BF16),
            jax.ShapeDtypeStruct(cotangent.shape, BF16),
            jax.ShapeDtypeStruct(weight.shape, F32),
        ],
    )(*terms, weight, cotangent)


def final_kernel(n_terms, *refs):
    terms, out_ref = refs[:n_terms], refs[n_terms]
    for t in range(out_ref.shape[0]):
        total = terms[0][t].astype(F32)
        for term in terms[1:]:
            total = total + term[t].astype(F32)
        out_ref[t] = total.T.astype(BF16)


def final(terms):
    return pl.pallas_call(
        functools.partial(final_kernel, len(terms)),
        out_shape=jax.ShapeDtypeStruct(terms[0].shape, BF16),
    )(*terms)


def shards(features, weight, adj_tiles, tile_rows, tile_cols, tile_count, cotangent):
    node_dev, width = features.shape
    tile_size = adj_tiles.shape[1]
    dev_tiles = node_dev // tile_size
    as_tiles = (dev_tiles, tile_size, width)
    row_id = lax.axis_index("row").astype(jnp.int32)
    col_id = lax.axis_index("col").astype(jnp.int32)
    inner = ((col_id // 2) % 4 == 1) | ((col_id // 2) % 4 == 2)
    inner = inner.astype(jnp.int32)
    table = (tile_rows, tile_cols, tile_count)
    group = gather_pieces(features.reshape(as_tiles), "row")
    parts = tile_pass(
        *table, jnp.stack([row_id, col_id, inner]), adj_tiles, group, lax.axis_size("col"), dev_tiles, True
    )
    terms = scatter_pieces(parts, "col")
    out_features, grad, wterm = middle(terms, weight, cotangent.reshape(as_tiles))
    panel = gather_pieces(grad, "col")
    weight_grad = all_sum(wterm, ("row", "col"))
    panel, weight_grad = lax.optimization_barrier((panel, weight_grad))
    parts = tile_pass(
        *table, jnp.stack([col_id, row_id, inner]), adj_tiles, panel, lax.axis_size("row"), dev_tiles, False
    )
    feature_grad = final(scatter_pieces(parts, "row"))
    return (
        out_features.reshape(node_dev, width),
        weight_grad,
        feature_grad.reshape(node_dev, width),
    )


def solution(mesh):
    in_specs = (
        P(("row", "col"), None),
        P(),
        P(("row", "col"), None, None),
        P(("row", "col")),
        P(("row", "col")),
        P(("row", "col")),
        P(("row", "col"), None),
    )
    out_specs = (P(("row", "col"), None), P(), P(("row", "col"), None))
    return jax.shard_map(shards, mesh=mesh, in_specs=in_specs, out_specs=out_specs, check_vma=False)
```
